32 devices in a mesh: data: 1 (over z), col: 4 (over y), row: 8 (over x, core).
Axes of the slice: x: 4, y: 4, z: 1, core: 2. Of those that a mesh axis runs over, the one named last changes fastest.
The devices are a block of a 4x4x8 slice.
Arguments:
- image: bfloat16 [256, 128, 4], P(('data', 'row'), 'col')
- w_enc1a: bfloat16 [3, 3, 4, 320], replicated
- b_enc1a: float32 [320], replicated
- w_enc1b: bfloat16 [3, 3, 320, 320], replicated
- b_enc1b: float32 [320], replicated
- w_enc2a: bfloat16 [3, 3, 320, 640], replicated
- b_enc2a: float32 [640], replicated
- w_enc2b: bfloat16 [3, 3, 640, 640], replicated
- b_enc2b: float32 [640], replicated
- w_mid_a: bfloat16 [3, 3, 640, 1280], replicated
- b_mid_a: float32 [1280], replicated
- w_mid_b: bfloat16 [3, 3, 1280, 1280], replicated
- b_mid_b: float32 [1280], replicated
- w_up2: bfloat16 [2, 2, 1280, 640], replicated
- w_dec2a: bfloat16 [3, 3, 1280, 640], replicated
- b_dec2a: float32 [640], replicated
- w_dec2b: bfloat16 [3, 3, 640, 640], replicated
- b_dec2b: float32 [640], replicated
- w_up1: bfloat16 [2, 2, 640, 320], replicated
- w_dec1a: bfloat16 [3, 3, 640, 320], replicated
- b_dec1a: float32 [320], replicated
- w_dec1b: bfloat16 [3, 3, 320, 320], replicated
- b_dec1b: float32 [320], replicated
- w_head: bfloat16 [320, 4], replicated
- b_head: float32 [4], replicated
Outputs:
- output: float32 [256, 128, 4], P(('data', 'row'), 'col')
All inputs are finite; a program needn't handle non-finite values.
Results may differ from the reference program's by a relative error of at most 0.0171244.
Values are sent between devices in bfloat16 or wider.
A program may use at most 768 MiB of HBM per device.

```python
import jax
import jax.numpy as jnp
from jax import lax

IN_CH = 4
BASE_CH = 320
OUT_CH = 4
IMG_ROWS = 256
IMG_COLS = 128


def weight_specs():
    ch_one = BASE_CH
    ch_two = 2 * BASE_CH
    ch_four = 4 * BASE_CH
    bias_gain = 0.0625
    return [
        ("w_enc1a", (3, 3, IN_CH, ch_one), 9 * IN_CH, 2.0, jnp.bfloat16),
        ("b_enc1a", (ch_one,), 1, bias_gain, jnp.float32),
        ("w_enc1b", (3, 3, ch_one, ch_one), 9 * ch_one, 2.0, jnp.bfloat16),
        ("b_enc1b", (ch_one,), 1, bias_gain, jnp.float32),
        ("w_enc2a", (3, 3, ch_one, ch_two), 9 * ch_one, 2.0, jnp.bfloat16),
        ("b_enc2a", (ch_two,), 1, bias_gain, jnp.float32),
        ("w_enc2b", (3, 3, ch_two, ch_two), 9 * ch_two, 2.0, jnp.bfloat16),
        ("b_enc2b", (ch_two,), 1, bias_gain, jnp.float32),
        ("w_mid_a", (3, 3, ch_two, ch_four), 9 * ch_two, 2.0, jnp.bfloat16),
        ("b_mid_a", (ch_four,), 1, bias_gain, jnp.float32),
        ("w_mid_b", (3, 3, ch_four, ch_four), 9 * ch_four, 2.0, jnp.bfloat16),
        ("b_mid_b", (ch_four,), 1, bias_gain, jnp.float32),
        ("w_up2", (2, 2, ch_four, ch_two), ch_four, 1.0, jnp.bfloat16),
        ("w_dec2a", (3, 3, ch_four, ch_two), 9 * ch_four, 2.0, jnp.bfloat16),
        ("b_dec2a", (ch_two,), 1, bias_gain, jnp.float32),
        ("w_dec2b", (3, 3, ch_two, ch_two), 9 * ch_two, 2.0, jnp.bfloat16),
        ("b_dec2b", (ch_two,), 1, bias_gain, jnp.float32),
        ("w_up1", (2, 2, ch_two, ch_one), ch_two, 1.0, jnp.bfloat16),
        ("w_dec1a", (3, 3, ch_two, ch_one), 9 * ch_two, 2.0, jnp.bfloat16),
        ("b_dec1a", (ch_one,), 1, bias_gain, jnp.float32),
        ("w_dec1b", (3, 3, ch_one, ch_one), 9 * ch_one, 2.0, jnp.bfloat16),
        ("b_dec1b", (ch_one,), 1, bias_gain, jnp.float32),
        ("w_head", (ch_one, OUT_CH), ch_one, 1.0, jnp.bfloat16),
        ("b_head", (OUT_CH,), 1, bias_gain, jnp.float32),
    ]


def setup_inputs(seed: int = 0, part: int = 0) -> dict:
    root = jax.random.key(seed)
    image_key = jax.random.fold_in(jax.random.fold_in(root, 1000), part)
    pixels = jax.random.normal(image_key, (IMG_ROWS, IMG_COLS, IN_CH), jnp.float32)
    result = {"image": pixels.astype(jnp.bfloat16)}
    for index, spec in enumerate(weight_specs()):
        name, shape, fan_in, gain, dtype = spec
        values = jax.random.normal(jax.random.fold_in(root, index), shape, jnp.float32)
        result[name] = (values * (gain / fan_in) ** 0.5).astype(dtype)
    return result


def conv_relu(hidden, weight, bias):
    conv_out = lax.conv_general_dilated(hidden.astype(jnp.float32)[None], weight.astype(jnp.float32), (1, 1), "SAME", dimension_numbers=("NHWC", "HWIO", "NHWC"))[0]
    return jax.nn.relu(conv_out + bias).astype(jnp.bfloat16)


def double_conv(hidden, w_first, b_first, w_second, b_second):
    return conv_relu(conv_relu(hidden, w_first, b_first), w_second, b_second)


def max_pool(hidden):
    height, width, channels = hidden.shape
    return hidden.reshape(height // 2, 2, width // 2, 2, channels).max(axis=(1, 3))


def up_conv(hidden, weight):
    height = hidden.shape[0]
    width = hidden.shape[1]
    summed = jnp.einsum("ijc,abco->iajbo", hidden.astype(jnp.float32), weight.astype(jnp.float32))
    return summed.astype(jnp.bfloat16).reshape(2 * height, 2 * width, weight.shape[3])


def reference(image, w_enc1a, b_enc1a, w_enc1b, b_enc1b, w_enc2a, b_enc2a, w_enc2b, b_enc2b, w_mid_a, b_mid_a, w_mid_b, b_mid_b, w_up2, w_dec2a, b_dec2a, w_dec2b, b_dec2b, w_up1, w_dec1a, b_dec1a, w_dec1b, b_dec1b, w_head, b_head):
    skip_one = double_conv(image, w_enc1a, b_enc1a, w_enc1b, b_enc1b)
    skip_two = double_conv(max_pool(skip_one), w_enc2a, b_enc2a, w_enc2b, b_enc2b)
    middle = double_conv(max_pool(skip_two), w_mid_a, b_mid_a, w_mid_b, b_mid_b)
    hidden = double_conv(jnp.concatenate([up_conv(middle, w_up2), skip_two], axis=2), w_dec2a, b_dec2a, w_dec2b, b_dec2b)
    hidden = double_conv(jnp.concatenate([up_conv(hidden, w_up1), skip_one], axis=2), w_dec1a, b_dec1a, w_dec1b, b_dec1b)
    flat = hidden.reshape(-1, hidden.shape[2])
    head_out = jnp.dot(flat, w_head, preferred_element_type=jnp.float32) + b_head
    return head_out.reshape(hidden.shape[0], hidden.shape[1], w_head.shape[1])
```

```python
import functools

import jax
import jax.numpy as jnp
from jax import lax
from jax.experimental import pallas as pl
from jax.experimental.pallas import tpu as pltpu
from jax.sharding import PartitionSpec as P

F32 = jnp.float32
BF16 = jnp.bfloat16
LANE = 128
DIRS = ((-1, 0), (1, 0), (0, -1), (0, 1), (-1, -1), (-1, 1), (1, -1), (1, 1))


def lane_tiles(channels):
    return [(t, t * LANE, min(LANE, channels - t * LANE)) for t in range(-(-channels // LANE))]


def mm(lhs, rhs, transposed):
    contract = (((1,), (1 if transposed else 0,)), ((), ()))
    return lax.dot_general(lhs, rhs, contract, preferred_element_type=F32)


class Map:
    def __init__(self, index, height, width, channels, refs, small):
        self.index, self.height, self.width, self.channels = index, height, width, channels
        if not small:
            self.x, self.el, self.er, self.hl, self.hr, self.cs, self.cr = refs
            self.top, self.bottom = self.x.at[1], self.x.at[height]
            self.above, self.below = self.x.at[0], self.x.at[height + 1]
        else:
            self.top, self.bottom, self.above, self.below, self.el, self.er, self.hl, self.hr, self.cs, self.cr = refs

    def copy_refs(self, d):
        return (
            (self.top, self.below), (self.bottom, self.above), (self.el, self.hr), (self.er, self.hl),
            (self.cs.at[0], self.cr.at[3]), (self.cs.at[1], self.cr.at[2]),
            (self.cs.at[2], self.cr.at[1]), (self.cs.at[3], self.cr.at[0]),
        )[d]

    def landing(self, dr, dc):
        if dc == 0:
            return self.above if dr < 0 else self.below
        if dr == 0:
            return self.hl if dc < 0 else self.hr
        return self.cr.at[(dr > 0) * 2 + (dc > 0)]


def map_scratch(height, width, channels, small):
    if small:
        shapes = [(2, width, channels)] * 4 + [(2, height, channels)] * 4 + [(4, 4, channels)] * 2
    else:
        shapes = [(height + 2, width, channels)] + [(height, channels)] * 4 + [(4, 2, channels)] * 2
    return [pltpu.VMEM(shape, BF16) for shape in shapes]


def map_specs(h1, w1, cin0, c1, c2):
    h2, w2 = h1 // 2, w1 // 2
    one, two = (h1, w1, c1, False), (h2, w2, c2, False)
    return [(h1, w1, cin0, False), one, (h2, w2, c1, False), two, (h2 // 2, w2 // 2, c2, True), two, two, two, one, one, one]


def split(cin):
    main = cin // 256 * 256
    return main, cin - main


def packed_lhs(slabs, cin):
    main, rest = split(cin)
    parts = [slab[:, :main] for slab in slabs] if main else []
    return parts + ([jnp.concatenate([slab[:, main:cin] for slab in slabs], axis=1)] if rest else [])


ALL_ROWS = (0, 1, 2)


def packed_rhs(piece, cin, axis, dys):
    main, rest = split(cin)
    parts = [piece(dy, 0, main) for dy in dys] if main else []
    return parts + ([jnp.concatenate([piece(dy, main, cin) for dy in dys], axis=axis)] if rest else [])


class Taps:
    transposed = False

    def __init__(self, buf, cin, cout, first=0, fold=1, rest=None):
        self.buf, self.cin, self.cout, self.first, self.fold, self.packed = buf, cin, cout, first, fold, rest
        self.main, self.rest = split(cout)

    def piece(self, dy, dx, k0, k1, n0, n1):
        tap = self.first + (dy * 3 + dx) * self.fold
        if self.fold > 1:
            return self.buf[pl.ds(tap, self.fold), :, n0:n1].reshape(self.cin, n1 - n0)[k0:k1]
        return self.buf[tap, k0:k1, n0:n1]

    def columns(self, dx, dys=ALL_ROWS):
        return packed_rhs(lambda dy, k0, k1: self.piece(dy, dx, k0, k1, 0, self.main), self.cin, 0, dys)

    def whole(self, dx, dys=ALL_ROWS):
        return packed_rhs(lambda dy, k0, k1: self.piece(dy, dx, k0, k1, 0, self.cout), self.cin, 0, dys)

    def last_columns(self, dys=ALL_ROWS):
        def piece(dy, k0, k1):
            if self.packed is not None:
                return self.packed[dy, k0:k1, :3 * self.rest]
            return jnp.concatenate([self.piece(dy, dx, k0, k1, self.main, self.cout) for dx in range(3)], axis=1)
        return packed_rhs(piece, self.cin, 0, dys)

    def pack(self):
        for dy in range(3):
            for dx in range(3):
                self.packed[dy, :, dx * self.rest:(dx + 1) * self.rest] = self.piece(dy, dx, 0, self.cin, self.main,
                                                                                     self.cout)


class TapsT(Taps):
    transposed = True

    def __init__(self, buf, cin, cout, lanes):
        super().__init__(buf, cin, cout)
        self.lanes = lanes

    def piece(self, dy, dx, k0, k1, n0, n1):
        start = self.lanes[k0 > 0]
        return self.buf[dy * 3 + dx, n0:n1, start:start + k1 - k0]

    def columns(self, dx, dys=ALL_ROWS):
        return packed_rhs(lambda dy, k0, k1: self.piece(dy, dx, k0, k1, 0, self.main), self.cin, 1, dys)

    def whole(self, dx, dys=ALL_ROWS):
        return packed_rhs(lambda dy, k0, k1: self.piece(dy, dx, k0, k1, 0, self.cout), self.cin, 1, dys)

    def last_columns(self, dys=ALL_ROWS):
        def piece(dy, k0, k1):
            return jnp.concatenate([self.piece(dy, dx, k0, k1, self.main, self.cout) for dx in range(3)], axis=0)
        return packed_rhs(piece, self.cin, 1, dys)


class TapsFirst(Taps):
    def __init__(self, stacked, stacked_rest, cin, cout):
        self.stacked, self.stacked_rest, self.cin, self.cout = stacked, stacked_rest, cin, cout
        self.main, self.rest = split(cout)

    def columns(self, dx, dys=ALL_ROWS):
        return [self.stacked[dx, :3 * self.cin, :self.main]]

    def whole(self, dx, dys=ALL_ROWS):
        return [self.stacked[dx, :3 * self.cin, :]]

    def last_columns(self, dys=ALL_ROWS):
        return [self.stacked_rest[:3 * self.cin, :3 * self.rest]]


def dots(lhs, rhs, transposed):
    total = mm(lhs[0], rhs[0], transposed)
    for a, b in zip(lhs[1:], rhs[1:]):
        total = total + mm(a, b, transposed)
    return total


def unet_kernel(cfg, image, w1a, b1a_, w1b, b1b_, w2a, b2a_, w2b, b2b_, wma, bma_, wmb, bmb_, wu2, wd2a, bd2a_, wd2b,
                bd2b_, wu1, wd1a, bd1a_, wd1b, bd1b_, wh, bh, out, *scratch):
    h1, w1, cin0, c1, c2, c3, rows, cols = cfg
    h2, w2, h3, w3 = h1 // 2, w1 // 2, h1 // 4, w1 // 4
    half = c3 // 2
    refs = list(scratch)

    def take(n):
        got = refs[:n]
        del refs[:n]
        return got

    maps = []
    for h, w, c, small in map_specs(h1, w1, cin0, c1, c2):
        maps.append(Map(len(maps), h, w, c, take(len(map_scratch(h, w, c, small))), small))
    mx, ma1, mp1, ma2, mp2, ms2, mu2, md2, ms1, mu1, md1 = maps
    (acc1, acc2, acc_skip, bscr, tscr, sides, f3, x3, x3b, m3, d2buf, buf_a, buf_b, buf_c, buf_d, buf_e, buf_f, rest_a, stacked, stacked_rest,
     buf_1a, b1a, b1b, b2a, b2b, bma, bmb, bd2a, bd2b, bd1a, bd1b, send_sem, recv_sem, load_sem) = refs

    data = lax.axis_index("data")
    my_col = lax.axis_index("col")
    my_row = lax.axis_index("row")

    def has(dr, dc):
        r, c = my_row + dr, my_col + dc
        return (r >= 0) & (r < rows) & (c >= 0) & (c < cols)

    def peer(dr, dc):
        return (data, my_col + dc, my_row + dr)

    biases = ((b1a_, b1a), (b1b_, b1b), (b2a_, b2a), (b2b_, b2b), (bma_, bma), (bmb_, bmb), (bd2a_, bd2a), (bd2b_, bd2b),
              (bd1a_, bd1a), (bd1b_, bd1b))
    loads = {
        "1a": (w1a, buf_1a),
        "1b": (w1b, buf_a),
        "2a": (w2a, buf_b),
        "2b": (w2b, buf_c),
        "ma0": (wma.at[:, :, :half], buf_d.at[:9]),
        "ma1": (wma.at[:, :, half:c3], buf_d.at[9:18]),
        "mb0": (wmb.at[:, :, :half], buf_e),
        "mb1": (wmb.at[:9, :, half:c3], buf_d.at[:9]),
        "mb2": (wmb.at[9:18, :, half:c3], buf_d.at[9:18]),
        "u2": (wu2, buf_c.at[:8]),
        "d2s": (wd2a.at[:, c2:2 * c2, :], buf_f),
        "d2u": (wd2a.at[:, :c2, :], buf_e.at[:9]),
        "d2b": (wd2b, buf_d.at[:9]),
        "u1": (wu1, buf_d.at[9:11]),
        "d1a": (wd1a, buf_b),
        "d1b": (wd1b, buf_a),
    }
    for i, pair in enumerate(biases):
        loads[i] = pair
    order = list(loads)

    def load(name):
        src, dst = loads[name]
        return pltpu.make_async_copy(src, dst, load_sem.at[order.index(name)])

    def remote(m, d):
        src, dst = m.copy_refs(d)
        return pltpu.make_async_remote_copy(src_ref=src, dst_ref=dst, send_sem=send_sem.at[m.index, d],
                                            recv_sem=recv_sem.at[m.index, d], device_id=peer(*DIRS[d]),
                                            device_id_type=pl.DeviceIdType.MESH)

    def send(m):
        for d in range(8):
            @pl.when(has(*DIRS[d]))
            def _(d=d):
                remote(m, d).start()

    def receive(m, which):
        for d in which:
            @pl.when(has(-DIRS[d][0], -DIRS[d][1]))
            def _(d=d):
                remote(m, d).wait_recv()

    ROWS, COLS = range(2), range(2, 8)

    load("1a").start()
    for i in range(len(biases)):
        load(i).start()
    load("1b").start()
    load("2a").start()
    load("2b").start()

    barrier = pltpu.get_barrier_semaphore()
    for dr, dc in DIRS:
        @pl.when(has(dr, dc))
        def _(dr=dr, dc=dc):
            pl.semaphore_signal(barrier, inc=1, device_id=peer(dr, dc), device_id_type=pl.DeviceIdType.MESH)

    def put_edges(m, acc, lanes=None):
        for t, lo, n in lane_tiles(m.channels):
            tile = acc.at[t]
            left = tile[pl.ds(0, m.height, stride=m.width), :]
            right = tile[pl.ds(m.width - 1, m.height, stride=m.width), :]
            put_columns(m, slice(0, m.height), left, right, (lanes or in_order)(t, lo, n))
            ends = (left[:1], right[:1], left[m.height - 1:], right[m.height - 1:])
            put_corners(m, ends, (lanes or in_order)(t, lo, n))

    def in_order(t, lo, n):
        return [(0, n, lo)]

    def rest_last(t, lo, n):
        rest = split(c1)[1]
        if t == 0:
            return [(rest, n, 0), (0, rest, c1 - rest)]
        return [(0, n, lo - rest)]

    def put_columns(m, rows_, left, right, lanes):
        for a, b, to in lanes:
            m.el[rows_, to:to + b - a] = left[:, a:b].astype(BF16)
            m.er[rows_, to:to + b - a] = right[:, a:b].astype(BF16)

    def put_corners(m, ends, lanes):
        for a, b, to in lanes:
            for k, pixel in enumerate(ends):
                m.cs[k, :, to:to + b - a] = jnp.broadcast_to(pixel[:, a:b], (2, b - a)).astype(BF16)

    def halo_slabs(m, side):
        h, cin = m.height, m.channels
        tscr[8:8 + h, :cin] = (m.hr if side else m.hl)[...].astype(F32)
        tscr[7:8, :cin] = m.cr[side].astype(F32)[:1]
        tscr[8 + h:9 + h, :cin] = m.cr[2 + side].astype(F32)[:1]
        return [tscr[7 + dy:7 + dy + h, :cin].astype(BF16) for dy in range(3)]

    def combine(px, w, cout, put):
        main, rest = split(cout)
        col = lax.broadcasted_iota(jnp.int32, (px, 1), 0) % w

        def shifted(left, right):
            return (jnp.where(col == 0, 0.0, pltpu.roll(left, 1, 0))
                    + jnp.where(col == w - 1, 0.0, pltpu.roll(right, px - 1, 0)))

        for t in range(main // LANE):
            lanes = slice(t * LANE, (t + 1) * LANE)
            put(t, bscr[1, :px, lanes] + shifted(bscr[0, :px, lanes], bscr[2, :px, lanes]))
        t = main // LANE
        if rest == LANE:
            put(t, bscr[3, :px, LANE:2 * LANE] + shifted(bscr[3, :px, :LANE], bscr[3, :px, 2 * LANE:3 * LANE]))
        else:
            pair = bscr[3, :px, :LANE]
            put(t, (pltpu.roll(pair, rest, 1) + shifted(pair, bscr[3, :px, LANE:2 * LANE]))[:, :rest])

    def large_sum(m, taps, cout, acc, add=False):
        h, w, cin = m.height, m.width, m.channels
        block = 8
        blocks = h // block
        px = block * w
        main, rest = split(cout)

        def one_block(i, carry):
            b = (i + 1) % blocks

            @pl.when(i == blocks - 2)
            def _():
                receive(m, ROWS)

            lhs = packed_lhs([m.x[pl.ds(b * block + dy, block)].reshape(px, cin) for dy in range(3)], cin)
            for dx in range(3):
                bscr[dx, :px, :main] = dots(lhs, taps.columns(dx), taps.transposed)
            bscr[3, :px, :3 * rest] = dots(lhs, taps.last_columns(), taps.transposed)

            def put(t, value):
                place = (t, pl.ds(b * px, px), slice(0, value.shape[1]))
                acc[place] = value + acc[place] if add else value
            combine(px, w, cout, put)
            return carry

        lax.fori_loop(0, blocks, one_block, 0)
        receive(m, COLS)
        for side, dx, at in ((0, 0, 0), (1, 2, w - 1)):
            tscr[:h, :cout] = dots(packed_lhs(halo_slabs(m, side), cin), taps.whole(dx), taps.transposed)
            for t, lo, n in lane_tiles(cout):
                tile = acc.at[t]
                tile[pl.ds(at, h, stride=w), :] += tscr[:h, lo:lo + LANE]

    def conv_large(m, taps, cout, acc, bias, store, add=False):
        large_sum(m, taps, cout, acc, add)
        block = 8
        px = block * m.width

        def finish(b, carry):
            for t, lo, n in lane_tiles(cout):
                rows_ = pl.ds(b * px, px)
                value = jnp.maximum(acc[t, rows_, :n] + bias[lo:lo + n][None, :], 0.0)
                acc[t, rows_, :n] = value
                store(b * block, block, t, value)
            return carry

        lax.fori_loop(0, m.height // block, finish, 0)

    def conv_sum(m, taps, cout, tile_at, dys=ALL_ROWS, halo=True, add=False):
        h, w, cin = m.height, m.width, m.channels
        px = h * w
        count = px + 2 * h if halo else px
        main, rest = split(cout)
        late = [dy for dy in ALL_ROWS if dy not in dys] if halo else []
        if halo:
            receive(m, range(8))
            for side in range(2):
                for dy, part in enumerate(halo_slabs(m, side)):
                    sides[dy, side * h:(side + 1) * h, :cin] = part

        def lhs():
            def slab(dy):
                own_rows = m.x[dy:dy + h].reshape(px, cin)
                return jnp.concatenate([own_rows, sides[dy, :, :cin]], axis=0) if halo else own_rows
            return packed_lhs([slab(dy) for dy in dys], cin)

        def late_lhs():
            return packed_lhs([sides[dy, :, :cin] for dy in late], cin)

        def step(dx, carry):
            bscr[dx, :count, :main] = dots(lhs(), taps.columns(dx, dys), taps.transposed)
            if late:
                bscr[dx, px:count, :main] += dots(late_lhs(), taps.columns(dx, late), taps.transposed)
            return carry

        lax.fori_loop(0, 3, step, 0)
        bscr[3, :count, :3 * rest] = dots(lhs(), taps.last_columns(dys), taps.transposed)
        if late:
            bscr[3, px:count, :3 * rest] += dots(late_lhs(), taps.last_columns(late), taps.transposed)

        def put(t, value):
            ref, begin = tile_at(t)
            if add:
                value = value + ref[begin:begin + px, :]
            ref[begin:begin + px, :] = value
        combine(px, w, cout, put)
        if not halo:
            return
        for t, lo, n in lane_tiles(cout):
            ref, begin = tile_at(t)
            if lo < main:
                from_left, from_right = bscr[0, px:px + h, lo:lo + n], bscr[2, px + h:px + 2 * h, lo:lo + n]
            else:
                from_left, from_right = bscr[3, px:px + h, :n], bscr[3, px + h:px + 2 * h, 2 * n:3 * n]
            ref[pl.ds(begin, h, stride=w), :] += from_left
            ref[pl.ds(begin + w - 1, h, stride=w), :] += from_right

    def conv_mid(m, taps, cout, bias, store, partial=None):
        conv_sum(m, taps, cout, lambda t: (acc2.at[t], 0))
        for t, lo, n in lane_tiles(cout):
            total = acc2[t] + bias[lo:lo + n][None, :]
            if partial is not None:
                ref, first = partial(t)
                total = total + ref[first:first + h2 * w2, :]
            value = jnp.maximum(total, 0.0)
            acc2[t] = value
            store(0, h2, t, value)

    def keep_in(m, lanes=None):
        def store(first, count, t, value):
            for a, b, to in (lanes or in_order)(t, t * LANE, value.shape[1]):
                part = value[:, a:b].astype(BF16).reshape(count, m.width, b - a)
                m.x[pl.ds(1 + first, count), :, to:to + b - a] = part
        return store

    def pooled(acc, t, h, w):
        tile = acc.at[t]
        across = jnp.maximum(tile[pl.ds(0, h * w // 2, stride=2), :], tile[pl.ds(1, h * w // 2, stride=2), :])
        return across.reshape(h // 2, 2, w // 2, LANE).max(axis=1).reshape(h * w // 4, LANE)

    mx.x[1:h1 + 1] = image[...]
    acc1[0, :, :cin0] = image[...].reshape(h1 * w1, cin0).astype(F32)
    put_edges(mx, acc1)
    pl.semaphore_wait(barrier, sum(has(dr, dc).astype(jnp.int32) for dr, dc in DIRS))
    send(mx)

    for dr, dc in DIRS:
        @pl.when(jnp.logical_not(has(dr, dc)))
        def _(dr=dr, dc=dc):
            for m in maps:
                ref = m.landing(dr, dc)
                ref[...] = jnp.zeros(ref.shape, BF16)

    load("1a").wait()
    for i in range(len(biases)):
        load(i).wait()
    first = TapsFirst(stacked, stacked_rest, cin0, c1)
    depth = lax.broadcasted_iota(jnp.int32, (stacked.shape[1], cin0), 0)
    channel = lax.broadcasted_iota(jnp.int32, (stacked.shape[1], cin0), 1)
    for dx in range(3):
        total = 0.0
        for dy in range(3):
            place = jnp.where(depth == channel + dy * cin0, 1.0, 0.0).astype(BF16)
            total = total + mm(place, buf_1a[dy * 3 + dx], False)
        stacked[dx] = total.astype(BF16)
        stacked_rest[:, dx * first.rest:(dx + 1) * first.rest] = total[:, first.main:c1].astype(BF16)
    conv_large(mx, first, c1, acc1, b1a, keep_in(ma1))
    put_edges(ma1, acc1)
    send(ma1)
    load("ma0").start()
    load("ma1").start()
    load("1b").wait()
    taps = Taps(buf_a, c1, c1, rest=rest_a)
    taps.pack()
    conv_large(ma1, taps, c1, acc1, b1b, keep_in(ms1, rest_last))
    load("d1b").start()
    for t, lo, n in lane_tiles(c1):
        value = pooled(acc1, t, h1, w1)
        acc2[t] = value
        mp1.x[1:h2 + 1, :, lo:lo + n] = value[:, :n].astype(BF16).reshape(h2, w2, n)
    put_edges(mp1, acc2)
    send(mp1)
    put_edges(ms1, acc1, rest_last)
    send(ms1)
    load("mb0").start()

    load("2a").wait()
    conv_mid(mp1, Taps(buf_b, c1, c2), c2, b2a, keep_in(ma2))
    put_edges(ma2, acc2)
    send(ma2)
    load("d1a").start()
    load("d2s").start()
    load("2b").wait()
    conv_mid(ma2, Taps(buf_c, c2, c2), c2, b2b, keep_in(ms2))
    load("u2").start()

    stride = 2 * w3
    own = h3 * stride
    wide = (h3 + 2) * stride

    def at_pixel(r, c):
        return (r + 2) * stride + c + 2

    def send_small(m):
        for t, lo, n in lane_tiles(m.channels):
            tile = f3.at[t]
            lanes = slice(lo, lo + n)
            for k in range(2):
                def run(r, c, count):
                    return tile[at_pixel(r, c):at_pixel(r, c) + count, :].astype(BF16)

                def column(c):
                    return tile[pl.ds(at_pixel(0, c), h3, stride=stride), :].astype(BF16)

                m.top[k, :, lanes] = run(k, 0, w3)
                m.bottom[k, :, lanes] = run(h3 - 2 + k, 0, w3)
                m.el[k, :, lanes] = column(k)
                m.er[k, :, lanes] = column(w3 - 2 + k)
                for corner, (r, c) in enumerate(((0, 0), (0, w3 - 2), (h3 - 2, 0), (h3 - 2, w3 - 2))):
                    m.cs[corner, 2 * k:2 * k + 2, lanes] = run(r + k, c, 2)
        send(m)

    def assemble_small(m):
        receive(m, range(8))
        for t, lo, n in lane_tiles(m.channels):
            tile = f3.at[t]
            lanes = slice(lo, lo + n)
            for k in range(2):
                def put_run(r, c, value):
                    tile[at_pixel(r, c):at_pixel(r, c) + value.shape[0], :] = value.astype(F32)

                put_run(k - 2, 0, m.above[k, :, lanes])
                put_run(h3 + k, 0, m.below[k, :, lanes])
                tile[pl.ds(at_pixel(0, k - 2), h3, stride=stride), :] = m.hl[k, :, lanes].astype(F32)
                tile[pl.ds(at_pixel(0, w3 + k), h3, stride=stride), :] = m.hr[k, :, lanes].astype(F32)
                for corner, (r, c) in enumerate(((-2, -2), (-2, w3), (h3, -2), (h3, w3))):
                    put_run(r + k, c, m.cr[corner, :, lanes].astype(F32)[2 * k:2 * k + 2])
            x3[:, lanes] = tile[...].astype(BF16)

    def conv_small(src, count, cin, taps, bias, which, store):
        main, rest = split(half)

        def lhs():
            return packed_lhs([src[dy * stride:dy * stride + count, :] for dy in range(3)], cin)

        def step(dx, carry):
            bscr[dx, :count, :main] = dots(lhs(), taps.columns(dx), False)
            return carry

        lax.fori_loop(0, 3, step, 0)
        bscr[3, :count, :3 * rest] = dots(lhs(), taps.last_columns(), False)
        for t, lo, n in lane_tiles(half):
            if lo < main:
                parts = [bscr[dx, :count, lo:lo + n] for dx in range(3)]
            else:
                parts = [bscr[3, :count, dx * rest:(dx + 1) * rest] for dx in range(3)]
            value = parts[0] + pltpu.roll(parts[1], count - 1, 0) + pltpu.roll(parts[2], count - 2, 0)
            at = which * half + lo
            store(at, jnp.maximum(value + bias[at:at + n][None, :], 0.0))

    for t, lo, n in lane_tiles(c2):
        value = pooled(acc2, t, h2, w2)
        for r in range(h3):
            f3[t, at_pixel(r, 0):at_pixel(r, 0) + w3, :] = value[r * w3:(r + 1) * w3]
    send_small(mp2)
    put_edges(ms2, acc2)
    send(ms2)

    def skip_sum(t):
        return acc_skip.at[t], 0

    load("d2s").wait()
    skip_taps = Taps(buf_f, c2, c2)
    conv_sum(ms2, skip_taps, c2, skip_sum, dys=(1,), halo=False)
    load("ma0").wait()
    load("ma1").wait()
    assemble_small(mp2)

    place = lax.broadcasted_iota(jnp.int32, (wide, 1), 0)
    line, spot = place // stride, place % stride
    inside = ((line >= 1 - has(-1, 0).astype(jnp.int32)) & (line <= h3 + has(1, 0).astype(jnp.int32))
              & (spot >= 1 - has(0, -1).astype(jnp.int32)) & (spot <= w3 + has(0, 1).astype(jnp.int32)))

    def keep_padded(lo, value):
        x3b[:, lo:lo + LANE] = jnp.where(inside, value, 0.0).astype(BF16)

    def keep_flat(lo, value):
        m3[:, lo:lo + LANE] = value.astype(BF16)

    for which in range(2):
        conv_small(x3, wide, c2, Taps(buf_d, c2, half, first=9 * which), bma, which, keep_padded)
        load(("mb1", "mb2")[which]).start()
    load("mb0").wait()
    conv_small(x3b, own, c3, Taps(buf_e, c3, half, fold=2), bmb, 0, keep_flat)
    load("d2u").start()
    load("mb1").wait()
    load("mb2").wait()
    conv_small(x3b, own, c3, Taps(buf_d, c3, half, fold=2), bmb, 1, keep_flat)
    load("d2b").start()
    load("u1").start()

    load("u2").wait()
    for p in range(2):
        for q in range(2):
            at = 2 * (2 * p + q)
            value = mm(m3[...], buf_c[at:at + 2].reshape(c3, c2), False)
            for t, lo, n in lane_tiles(c2):
                bscr[0, :own, :LANE] = value[:, lo:lo + n]
                tile = acc2.at[t]
                for r in range(h3):
                    tile[pl.ds((2 * r + p) * w2 + q, w3, stride=2), :] = bscr[0, r * stride:r * stride + w3, :LANE]
    for t, lo, n in lane_tiles(c2):
        mu2.x[1:h2 + 1, :, lo:lo + n] = acc2[t].astype(BF16).reshape(h2, w2, n)
    put_edges(mu2, acc2)
    send(mu2)
    conv_sum(ms2, skip_taps, c2, skip_sum, dys=(0, 2), add=True)
    load("d2u").wait()
    conv_mid(mu2, Taps(buf_e, c2, c2), c2, bd2a, keep_in(md2), partial=skip_sum)
    put_edges(md2, acc2)
    send(md2)
    load("d1a").wait()
    large_sum(ms1, TapsT(buf_b, c1, c1, (2 * c1 - split(c1)[0], c1)), c1, acc1)
    load("d2b").wait()

    def keep_d2(begin, count, t, value):
        d2buf[:, t * LANE:(t + 1) * LANE] = value.astype(BF16)

    conv_mid(md2, Taps(buf_d, c2, c2), c2, bd2b, keep_d2)

    load("u1").wait()
    for at in range(4):
        bscr[at, :h2 * w2, :c1] = mm(d2buf[...], buf_d[9 + at // 2, (at % 2) * c1:(at % 2 + 1) * c1, :], True)
    quarter = h1 // 4
    for t, lo, n in lane_tiles(c1):
        for r in range(h2):
            tile = acc2.at[2 * r // quarter]
            for at in range(4):
                begin = (2 * r % quarter + at // 2) * w1 + at % 2
                tile[pl.ds(begin, w2, stride=2), :] = bscr[at, r * w2:(r + 1) * w2, lo:lo + LANE]
        ends = []
        for k in range(4):
            tile = acc2.at[k]
            mu1.x[1 + k * quarter:1 + (k + 1) * quarter, :, lo:lo + n] = tile[:, :n].astype(BF16).reshape(quarter, w1, n)
            left = tile[pl.ds(0, quarter, stride=w1), :]
            right = tile[pl.ds(w1 - 1, quarter, stride=w1), :]
            put_columns(mu1, slice(k * quarter, (k + 1) * quarter), left, right, in_order(t, lo, n))
            ends.append((left, right))
        (first_left, first_right), (last_left, last_right) = ends[0], ends[-1]
        put_corners(mu1, (first_left[:1], first_right[:1], last_left[quarter - 1:], last_right[quarter - 1:]),
                    in_order(t, lo, n))
    send(mu1)
    load("d1b").wait()
    taps.pack()
    conv_large(mu1, TapsT(buf_b, c1, c1, (0, split(c1)[0])), c1, acc1, bd1a, keep_in(md1), add=True)
    put_edges(md1, acc1)
    send(md1)

    def keep_last(begin, count, t, value):
        lo = t * LANE
        ma1.x[pl.ds(1 + begin, count), :, lo:lo + value.shape[1]] = value.astype(BF16).reshape(count, w1, value.shape[1])

    for d in range(8):
        @pl.when(has(*DIRS[d]))
        def _(d=d):
            remote(ma1, d).wait_send()
    conv_large(md1, taps, c1, acc1, bd1b, keep_last)

    for b in range(4):
        count = h1 // 4
        last = ma1.x[1 + b * count:1 + (b + 1) * count].reshape(count * w1, c1)
        y = mm(wh[...], last, True)
        for r in range(count):
            for o in range(wh.shape[0]):
                out[b * count + r, o:o + 1] = y[o:o + 1, r * w1:(r + 1) * w1] + bh[o]

    for m in maps:
        if m is ma1:
            continue
        for d in range(8):
            @pl.when(has(*DIRS[d]))
            def _(m=m, d=d):
                remote(m, d).wait_send()


def solution(mesh):
    rows, cols = mesh.shape["row"], mesh.shape["col"]
    tile_spec = P(("data", "row"), "col", None)

    def device_body(image, w1a, b1a, w1b, b1b, w2a, b2a, w2b, b2b, wma, bma, wmb, bmb, wu2, wd2a, bd2a, wd2b, bd2b,
                    wu1, wd1a, bd1a, wd1b, bd1b, wh, bh):
        h1, w1, cin = image.shape
        c1, c2, c3 = w1b.shape[3], w2b.shape[3], wmb.shape[3]
        couts = wh.shape[1]
        h2, w2, h3, w3 = h1 // 2, w1 // 2, h1 // 4, w1 // 4

        def stack(w):
            return w.reshape(-1, min(w.shape[2], c2), w.shape[3])

        def stack_t(w):
            return jnp.swapaxes(w, 2, 3).reshape(-1, w.shape[3], w.shape[2])

        operands = [image, w1a.reshape(9, cin, c1), b1a, stack(w1b), b1b, stack(w2a), b2a, stack(w2b), b2b,
                    stack(wma), bma, stack(wmb), bmb, stack(wu2), wd2a.reshape(9, 2 * c2, c2), bd2a, stack(wd2b), bd2b,
                    stack_t(wu1).reshape(2, 2 * c1, c2), stack_t(wd1a), bd1a, stack(wd1b), bd1b, wh.T, bh]
        in_vmem = {0, 23, 24}
        vmem = pl.BlockSpec(memory_space=pltpu.VMEM)
        hbm = pl.BlockSpec(memory_space=pl.ANY)
        nt1, nt2 = -(-c1 // LANE), c2 // LANE
        small = 2 * w3
        specs = map_specs(h1, w1, cin, c1, c2)
        scratch = (
            [shape for spec in specs for shape in map_scratch(*spec)]
            + [
                pltpu.VMEM((nt1, h1 * w1, LANE), F32), *[pltpu.VMEM((nt2, h2 * w2, LANE), F32)] * 2,
                pltpu.VMEM((4, h2 * w2 + 2 * h2, split(c2)[0]), F32), pltpu.VMEM((h1 + 16, c2), F32),
                pltpu.VMEM((3, 2 * h2, c2), BF16),
                pltpu.VMEM((nt2, (h3 + 4) * small, LANE), F32), pltpu.VMEM(((h3 + 4) * small, c2), BF16),
                pltpu.VMEM(((h3 + 2) * small, c3), BF16),
                pltpu.VMEM((h3 * small, c3), BF16), pltpu.VMEM((h2 * w2, c2), BF16),
                pltpu.VMEM((9, c1, c1), BF16), pltpu.VMEM((9, c1, c2), BF16), pltpu.VMEM((9, c2, c2), BF16),
                pltpu.VMEM((18, c2, c2), BF16), pltpu.VMEM((18, c2, c2), BF16), pltpu.VMEM((9, c2, c2), BF16),
                pltpu.VMEM((3, c1, 3 * split(c1)[1]), BF16),
                pltpu.VMEM((3, 16, c1), BF16), pltpu.VMEM((16, 3 * split(c1)[1]), BF16),
                pltpu.VMEM((9, cin, c1), BF16),
                *[pltpu.VMEM((c,), F32) for c in (c1, c1, c2, c2, c3, c3, c2, c2, c1, c1)],
                *[pltpu.SemaphoreType.DMA((len(specs), len(DIRS)))] * 2, pltpu.SemaphoreType.DMA((26,)),
            ]
        )
        y = pl.pallas_call(
            functools.partial(unet_kernel, (h1, w1, cin, c1, c2, c3, rows, cols)),
            out_shape=jax.ShapeDtypeStruct((h1, couts, w1), F32),
            in_specs=[vmem if i in in_vmem else hbm for i in range(24)] + [pl.BlockSpec(memory_space=pltpu.SMEM)],
            out_specs=vmem,
            scratch_shapes=scratch,
            compiler_params=pltpu.CompilerParams(collective_id=0, has_side_effects=True, vmem_limit_bytes=67043328),
            name="unet",
        )(*operands)
        return y.transpose(0, 2, 1)

    def program(image, *params):
        mapped = jax.shard_map(device_body, mesh=mesh, in_specs=(tile_spec,) + tuple([P()] * len(params)),
                               out_specs=tile_spec, check_vma=False)
        return mapped(image, *params)

    return program
```

```python
import functools

import jax
import jax.numpy as jnp
from jax import lax
from jax.experimental import pallas as pl
from jax.experimental.pallas import tpu as pltpu
from jax.sharding import PartitionSpec as P

F32 = jnp.float32
BF16 = jnp.bfloat16
LANE = 128
DIRS = ((-1, 0), (1, 0), (0, -1), (0, 1), (-1, -1), (-1, 1), (1, -1), (1, 1))


def lane_tiles(channels):
    return [(t, t * LANE, min(LANE, channels - t * LANE)) for t in range(-(-channels // LANE))]


def mm(lhs, rhs, transposed):
    contract = (((1,), (1 if transposed else 0,)), ((), ()))
    return lax.dot_general(lhs, rhs, contract, preferred_element_type=F32)


class Map:
    def __init__(self, index, height, width, channels, refs, small):
        self.index, self.height, self.width, self.channels = index, height, width, channels
        if not small:
            self.x, self.el, self.er, self.hl, self.hr, self.cs, self.cr = refs
            self.top, self.bottom = self.x.at[1], self.x.at[height]
            self.above, self.below = self.x.at[0], self.x.at[height + 1]
        else:
            self.top, self.bottom, self.above, self.below, self.el, self.er, self.hl, self.hr, self.cs, self.cr = refs

    def copy_refs(self, d):
        return (
            (self.top, self.below), (self.bottom, self.above), (self.el, self.hr), (self.er, self.hl),
            (self.cs.at[0], self.cr.at[3]), (self.cs.at[1], self.cr.at[2]),
            (self.cs.at[2], self.cr.at[1]), (self.cs.at[3], self.cr.at[0]),
        )[d]

    def landing(self, dr, dc):
        if dc == 0:
            return self.above if dr < 0 else self.below
        if dr == 0:
            return self.hl if dc < 0 else self.hr
        return self.cr.at[(dr > 0) * 2 + (dc > 0)]


def map_scratch(height, width, channels, small):
    if small:
        shapes = [(2, width, channels)] * 4 + [(2, height, channels)] * 4 + [(4, 4, channels)] * 2
    else:
        shapes = [(height + 2, width, channels)] + [(height, channels)] * 4 + [(4, 2, channels)] * 2
    return [pltpu.VMEM(shape, BF16) for shape in shapes]


def map_specs(h1, w1, cin0, c1, c2):
    h2, w2 = h1 // 2, w1 // 2
    one, two = (h1, w1, c1, False), (h2, w2, c2, False)
    return [(h1, w1, cin0, False), one, (h2, w2, c1, False), two, (h2 // 2, w2 // 2, c2, True), two, two, two, one, one, one]


def split(cin):
    main = cin // 256 * 256
    return main, cin - main


def packed_lhs(slabs, cin):
    main, rest = split(cin)
    parts = [slab[:, :main] for slab in slabs] if main else []
    return parts + ([jnp.concatenate([slab[:, main:cin] for slab in slabs], axis=1)] if rest else [])


ALL_ROWS = (0, 1, 2)


def packed_rhs(piece, cin, axis, dys):
    main, rest = split(cin)
    parts = [piece(dy, 0, main) for dy in dys] if main else []
    return parts + ([jnp.concatenate([piece(dy, main, cin) for dy in dys], axis=axis)] if rest else [])


class Taps:
    transposed = False

    def __init__(self, buf, cin, cout, first=0, fold=1, rest=None):
        self.buf, self.cin, self.cout, self.first, self.fold, self.packed = buf, cin, cout, first, fold, rest
        self.main, self.rest = split(cout)

    def piece(self, dy, dx, k0, k1, n0, n1):
        tap = self.first + (dy * 3 + dx) * self.fold
        if self.fold > 1:
            return self.buf[pl.ds(tap, self.fold), :, n0:n1].reshape(self.cin, n1 - n0)[k0:k1]
        return self.buf[tap, k0:k1, n0:n1]

    def columns(self, dx, dys=ALL_ROWS):
        return packed_rhs(lambda dy, k0, k1: self.piece(dy, dx, k0, k1, 0, self.main), self.cin, 0, dys)

    def whole(self, dx, dys=ALL_ROWS):
        return packed_rhs(lambda dy, k0, k1: self.piece(dy, dx, k0, k1, 0, self.cout), self.cin, 0, dys)

    def last_columns(self, dys=ALL_ROWS):
        def piece(dy, k0, k1):
            if self.packed is not None:
                return self.packed[dy, k0:k1, :3 * self.rest]
            return jnp.concatenate([self.piece(dy, dx, k0, k1, self.main, self.cout) for dx in range(3)], axis=1)
        return packed_rhs(piece, self.cin, 0, dys)

    def pack(self):
        for dy in range(3):
            for dx in range(3):
                self.packed[dy, :, dx * self.rest:(dx + 1) * self.rest] = self.piece(dy, dx, 0, self.cin, self.main,
                                                                                     self.cout)


class TapsT(Taps):
    transposed = True

    def __init__(self, buf, cin, cout, lanes):
        super().__init__(buf, cin, cout)
        self.lanes = lanes

    def piece(self, dy, dx, k0, k1, n0, n1):
        start = self.lanes[k0 > 0]
        return self.buf[dy * 3 + dx, n0:n1, start:start + k1 - k0]

    def columns(self, dx, dys=ALL_ROWS):
        return packed_rhs(lambda dy, k0, k1: self.piece(dy, dx, k0, k1, 0, self.main), self.cin, 1, dys)

    def whole(self, dx, dys=ALL_ROWS):
        return packed_rhs(lambda dy, k0, k1: self.piece(dy, dx, k0, k1, 0, self.cout), self.cin, 1, dys)

    def last_columns(self, dys=ALL_ROWS):
        def piece(dy, k0, k1):
            return jnp.concatenate([self.piece(dy, dx, k0, k1, self.main, self.cout) for dx in range(3)], axis=0)
        return packed_rhs(piece, self.cin, 1, dys)


class TapsFirst(Taps):
    def __init__(self, stacked, stacked_rest, cin, cout):
        self.stacked, self.stacked_rest, self.cin, self.cout = stacked, stacked_rest, cin, cout
        self.main, self.rest = split(cout)

    def columns(self, dx, dys=ALL_ROWS):
        return [self.stacked[dx, :3 * self.cin, :self.main]]

    def whole(self, dx, dys=ALL_ROWS):
        return [self.stacked[dx, :3 * self.cin, :]]

    def last_columns(self, dys=ALL_ROWS):
        return [self.stacked_rest[:3 * self.cin, :3 * self.rest]]


def dots(lhs, rhs, transposed):
    total = mm(lhs[0], rhs[0], transposed)
    for a, b in zip(lhs[1:], rhs[1:]):
        total = total + mm(a, b, transposed)
    return total


def unet_kernel(cfg, image, w1a, b1a_, w1b, b1b_, w2a, b2a_, w2b, b2b_, wma, bma_, wmb, bmb_, wu2, wd2a, bd2a_, wd2b,
                bd2b_, wu1, wd1a, bd1a_, wd1b, bd1b_, wh, bh, out, *scratch):
    h1, w1, cin0, c1, c2, c3, rows, cols = cfg
    h2, w2, h3, w3 = h1 // 2, w1 // 2, h1 // 4, w1 // 4
    half = c3 // 2
    refs = list(scratch)

    def take(n):
        got = refs[:n]
        del refs[:n]
        return got

    maps = []
    for h, w, c, small in map_specs(h1, w1, cin0, c1, c2):
        maps.append(Map(len(maps), h, w, c, take(len(map_scratch(h, w, c, small))), small))
    mx, ma1, mp1, ma2, mp2, ms2, mu2, md2, ms1, mu1, md1 = maps
    (acc1, acc2, acc_skip, bscr, tscr, sides, f3, x3, x3b, m3, d2buf, buf_a, buf_b, buf_c, buf_d, buf_e, buf_f, rest_a, stacked, stacked_rest,
     buf_1a, b1a, b1b, b2a, b2b, bma, bmb, bd2a, bd2b, bd1a, bd1b, send_sem, recv_sem, load_sem) = refs

    data = lax.axis_index("data")
    my_col = lax.axis_index("col")
    my_row = lax.axis_index("row")

    def has(dr, dc):
        r, c = my_row + dr, my_col + dc
        return (r >= 0) & (r < rows) & (c >= 0) & (c < cols)

    def peer(dr, dc):
        return (data, my_col + dc, my_row + dr)

    biases = ((b1a_, b1a), (b1b_, b1b), (b2a_, b2a), (b2b_, b2b), (bma_, bma), (bmb_, bmb), (bd2a_, bd2a), (bd2b_, bd2b),
              (bd1a_, bd1a), (bd1b_, bd1b))
    loads = {
        "1a": (w1a, buf_1a),
        "1b": (w1b, buf_a),
        "2a": (w2a, buf_b),
        "2b": (w2b, buf_c),
        "ma0": (wma.at[:, :, :half], buf_d.at[:9]),
        "ma1": (wma.at[:, :, half:c3], buf_d.at[9:18]),
        "mb0": (wmb.at[:, :, :half], buf_e),
        "mb1": (wmb.at[:9, :, half:c3], buf_d.at[:9]),
        "mb2": (wmb.at[9:18, :, half:c3], buf_d.at[9:18]),
        "u2": (wu2, buf_c.at[:8]),
        "d2s": (wd2a.at[:, c2:2 * c2, :], buf_f),
        "d2u": (wd2a.at[:, :c2, :], buf_e.at[:9]),
        "d2b": (wd2b, buf_d.at[:9]),
        "u1": (wu1, buf_d.at[9:11]),
        "d1a": (wd1a, buf_b),
        "d1s": (wd1a, buf_f.at[:, :c1]),
        "d1b": (wd1b, buf_a),
    }
    for i, pair in enumerate(biases):
        loads[i] = pair
    order = list(loads)

    def load(name):
        src, dst = loads[name]
        return pltpu.make_async_copy(src, dst, load_sem.at[order.index(name)])

    def remote(m, d):
        src, dst = m.copy_refs(d)
        return pltpu.make_async_remote_copy(src_ref=src, dst_ref=dst, send_sem=send_sem.at[m.index, d],
                                            recv_sem=recv_sem.at[m.index, d], device_id=peer(*DIRS[d]),
                                            device_id_type=pl.DeviceIdType.MESH)

    def send(m):
        for d in range(8):
            @pl.when(has(*DIRS[d]))
            def _(d=d):
                remote(m, d).start()

    def receive(m, which):
        for d in which:
            @pl.when(has(-DIRS[d][0], -DIRS[d][1]))
            def _(d=d):
                remote(m, d).wait_recv()

    ROWS, COLS = range(2), range(2, 8)

    load("1a").start()
    for i in range(len(biases)):
        load(i).start()
    load("1b").start()
    load("2a").start()
    load("2b").start()
    load("d1s").start()

    barrier = pltpu.get_barrier_semaphore()
    for dr, dc in DIRS:
        @pl.when(has(dr, dc))
        def _(dr=dr, dc=dc):
            pl.semaphore_signal(barrier, inc=1, device_id=peer(dr, dc), device_id_type=pl.DeviceIdType.MESH)

    def put_edges(m, acc, lanes=None):
        for t, lo, n in lane_tiles(m.channels):
            tile = acc.at[t]
            left = tile[pl.ds(0, m.height, stride=m.width), :]
            right = tile[pl.ds(m.width - 1, m.height, stride=m.width), :]
            put_columns(m, slice(0, m.height), left, right, (lanes or in_order)(t, lo, n))
            ends = (left[:1], right[:1], left[m.height - 1:], right[m.height - 1:])
            put_corners(m, ends, (lanes or in_order)(t, lo, n))

    def in_order(t, lo, n):
        return [(0, n, lo)]

    def rest_last(t, lo, n):
        rest = split(c1)[1]
        if t == 0:
            return [(rest, n, 0), (0, rest, c1 - rest)]
        return [(0, n, lo - rest)]

    def put_columns(m, rows_, left, right, lanes):
        for a, b, to in lanes:
            m.el[rows_, to:to + b - a] = left[:, a:b].astype(BF16)
            m.er[rows_, to:to + b - a] = right[:, a:b].astype(BF16)

    def put_corners(m, ends, lanes):
        for a, b, to in lanes:
            for k, pixel in enumerate(ends):
                m.cs[k, :, to:to + b - a] = jnp.broadcast_to(pixel[:, a:b], (2, b - a)).astype(BF16)

    def halo_slabs(m, side):
        h, cin = m.height, m.channels
        tscr[8:8 + h, :cin] = (m.hr if side else m.hl)[...].astype(F32)
        tscr[7:8, :cin] = m.cr[side].astype(F32)[:1]
        tscr[8 + h:9 + h, :cin] = m.cr[2 + side].astype(F32)[:1]
        return [tscr[7 + dy:7 + dy + h, :cin].astype(BF16) for dy in range(3)]

    def combine(px, w, cout, put):
        main, rest = split(cout)
        col = lax.broadcasted_iota(jnp.int32, (px, 1), 0) % w

        def shifted(left, right):
            return (jnp.where(col == 0, 0.0, pltpu.roll(left, 1, 0))
                    + jnp.where(col == w - 1, 0.0, pltpu.roll(right, px - 1, 0)))

        for t in range(main // LANE):
            lanes = slice(t * LANE, (t + 1) * LANE)
            put(t, bscr[1, :px, lanes] + shifted(bscr[0, :px, lanes], bscr[2, :px, lanes]))
        t = main // LANE
        if rest == LANE:
            put(t, bscr[3, :px, LANE:2 * LANE] + shifted(bscr[3, :px, :LANE], bscr[3, :px, 2 * LANE:3 * LANE]))
        else:
            pair = bscr[3, :px, :LANE]
            put(t, (pltpu.roll(pair, rest, 1) + shifted(pair, bscr[3, :px, LANE:2 * LANE]))[:, :rest])

    def large_sum(m, taps, cout, acc, add=False, interior=True, border=True):
        h, w, cin = m.height, m.width, m.channels
        block = 8
        blocks = h // block
        px = block * w
        main, rest = split(cout)

        def one_block(i, carry):
            b = (i + 1) % blocks

            @pl.when(i == blocks - 2)
            def _():
                receive(m, ROWS)

            lhs = packed_lhs([m.x[pl.ds(b * block + dy, block)].reshape(px, cin) for dy in range(3)], cin)
            for dx in range(3):
                bscr[dx, :px, :main] = dots(lhs, taps.columns(dx), taps.transposed)
            bscr[3, :px, :3 * rest] = dots(lhs, taps.last_columns(), taps.transposed)

            def put(t, value):
                place = (t, pl.ds(b * px, px), slice(0, value.shape[1]))
                acc[place] = value + acc[place] if add else value
            combine(px, w, cout, put)
            return carry

        lax.fori_loop(0 if interior else blocks - 2, blocks if border else blocks - 2, one_block, 0)
        if not border:
            return
        receive(m, COLS)
        for side, dx, at in ((0, 0, 0), (1, 2, w - 1)):
            tscr[:h, :cout] = dots(packed_lhs(halo_slabs(m, side), cin), taps.whole(dx), taps.transposed)
            for t, lo, n in lane_tiles(cout):
                tile = acc.at[t]
                tile[pl.ds(at, h, stride=w), :] += tscr[:h, lo:lo + LANE]

    def conv_large(m, taps, cout, acc, bias, store, add=False):
        large_sum(m, taps, cout, acc, add)
        block = 8
        px = block * m.width

        def finish(b, carry):
            for t, lo, n in lane_tiles(cout):
                rows_ = pl.ds(b * px, px)
                value = jnp.maximum(acc[t, rows_, :n] + bias[lo:lo + n][None, :], 0.0)
                acc[t, rows_, :n] = value
                store(b * block, block, t, value)
            return carry

        lax.fori_loop(0, m.height // block, finish, 0)

    def conv_sum(m, taps, cout, tile_at, dys=ALL_ROWS, halo=True, add=False):
        h, w, cin = m.height, m.width, m.channels
        px = h * w
        count = px + 2 * h if halo else px
        main, rest = split(cout)
        late = [dy for dy in ALL_ROWS if dy not in dys] if halo else []
        if halo:
            receive(m, range(8))
            for side in range(2):
                for dy, part in enumerate(halo_slabs(m, side)):
                    sides[dy, side * h:(side + 1) * h, :cin] = part

        def lhs():
            def slab(dy):
                own_rows = m.x[dy:dy + h].reshape(px, cin)
                return jnp.concatenate([own_rows, sides[dy, :, :cin]], axis=0) if halo else own_rows
            return packed_lhs([slab(dy) for dy in dys], cin)

        def late_lhs():
            return packed_lhs([sides[dy, :, :cin] for dy in late], cin)

        def step(dx, carry):
            bscr[dx, :count, :main] = dots(lhs(), taps.columns(dx, dys), taps.transposed)
            if late:
                bscr[dx, px:count, :main] += dots(late_lhs(), taps.columns(dx, late), taps.transposed)
            return carry

        for dx in range(3):
            step(dx, 0)
        bscr[3, :count, :3 * rest] = dots(lhs(), taps.last_columns(dys), taps.transposed)
        if late:
            bscr[3, px:count, :3 * rest] += dots(late_lhs(), taps.last_columns(late), taps.transposed)

        def put(t, value):
            ref, begin = tile_at(t)
            if add:
                value = value + ref[begin:begin + px, :]
            ref[begin:begin + px, :] = value
        combine(px, w, cout, put)
        if not halo:
            return
        for t, lo, n in lane_tiles(cout):
            ref, begin = tile_at(t)
            if lo < main:
                from_left, from_right = bscr[0, px:px + h, lo:lo + n], bscr[2, px + h:px + 2 * h, lo:lo + n]
            else:
                from_left, from_right = bscr[3, px:px + h, :n], bscr[3, px + h:px + 2 * h, 2 * n:3 * n]
            ref[pl.ds(begin, h, stride=w), :] += from_left
            ref[pl.ds(begin + w - 1, h, stride=w), :] += from_right

    def conv_mid(m, taps, cout, bias, store, partial=None):
        conv_sum(m, taps, cout, lambda t: (acc2.at[t], 0))
        for t, lo, n in lane_tiles(cout):
            total = acc2[t] + bias[lo:lo + n][None, :]
            if partial is not None:
                ref, first = partial(t)
                total = total + ref[first:first + h2 * w2, :]
            value = jnp.maximum(total, 0.0)
            acc2[t] = value
            store(0, h2, t, value)

    def keep_in(m, lanes=None):
        def store(first, count, t, value):
            for a, b, to in (lanes or in_order)(t, t * LANE, value.shape[1]):
                part = value[:, a:b].astype(BF16).reshape(count, m.width, b - a)
                m.x[pl.ds(1 + first, count), :, to:to + b - a] = part
        return store

    def pooled(acc, t, h, w):
        tile = acc.at[t]
        across = jnp.maximum(tile[pl.ds(0, h * w // 2, stride=2), :], tile[pl.ds(1, h * w // 2, stride=2), :])
        return across.reshape(h // 2, 2, w // 2, LANE).max(axis=1).reshape(h * w // 4, LANE)

    mx.x[1:h1 + 1] = image[...]
    acc1[0, :, :cin0] = image[...].reshape(h1 * w1, cin0).astype(F32)
    put_edges(mx, acc1)
    pl.semaphore_wait(barrier, sum(has(dr, dc).astype(jnp.int32) for dr, dc in DIRS))
    send(mx)

    for dr, dc in DIRS:
        @pl.when(jnp.logical_not(has(dr, dc)))
        def _(dr=dr, dc=dc):
            for m in maps:
                ref = m.landing(dr, dc)
                ref[...] = jnp.zeros(ref.shape, BF16)

    load("1a").wait()
    for i in range(len(biases)):
        load(i).wait()
    first = TapsFirst(stacked, stacked_rest, cin0, c1)
    depth = lax.broadcasted_iota(jnp.int32, (stacked.shape[1], cin0), 0)
    channel = lax.broadcasted_iota(jnp.int32, (stacked.shape[1], cin0), 1)
    for dx in range(3):
        total = 0.0
        for dy in range(3):
            place = jnp.where(depth == channel + dy * cin0, 1.0, 0.0).astype(BF16)
            total = total + mm(place, buf_1a[dy * 3 + dx], False)
        stacked[dx] = total.astype(BF16)
        stacked_rest[:, dx * first.rest:(dx + 1) * first.rest] = total[:, first.main:c1].astype(BF16)
    conv_large(mx, first, c1, acc1, b1a, keep_in(ma1))
    put_edges(ma1, acc1)
    send(ma1)
    load("ma0").start()
    load("ma1").start()
    load("1b").wait()
    taps = Taps(buf_a, c1, c1, rest=rest_a)
    taps.pack()
    conv_large(ma1, taps, c1, acc1, b1b, keep_in(ms1, rest_last))
    load("d1b").start()
    for t, lo, n in lane_tiles(c1):
        value = pooled(acc1, t, h1, w1)
        acc2[t] = value
        mp1.x[1:h2 + 1, :, lo:lo + n] = value[:, :n].astype(BF16).reshape(h2, w2, n)
    put_edges(mp1, acc2)
    send(mp1)
    put_edges(ms1, acc1, rest_last)
    send(ms1)
    load("d1s").wait()
    skip_one = TapsT(buf_f, c1, c1, (2 * c1 - split(c1)[0], c1))
    large_sum(ms1, skip_one, c1, acc1, border=False)
    load("mb0").start()

    load("2a").wait()
    conv_mid(mp1, Taps(buf_b, c1, c2), c2, b2a, keep_in(ma2))
    put_edges(ma2, acc2)
    send(ma2)
    load("d1a").start()
    large_sum(ms1, skip_one, c1, acc1, interior=False)
    load("d2s").start()
    load("2b").wait()
    conv_mid(ma2, Taps(buf_c, c2, c2), c2, b2b, keep_in(ms2))
    load("u2").start()

    stride = 2 * w3
    own = h3 * stride
    wide = (h3 + 2) * stride

    def at_pixel(r, c):
        return (r + 2) * stride + c + 2

    def send_small(m):
        for t, lo, n in lane_tiles(m.channels):
            tile = f3.at[t]
            lanes = slice(lo, lo + n)
            for k in range(2):
                def run(r, c, count):
                    return tile[at_pixel(r, c):at_pixel(r, c) + count, :].astype(BF16)

                def column(c):
                    return tile[pl.ds(at_pixel(0, c), h3, stride=stride), :].astype(BF16)

                m.top[k, :, lanes] = run(k, 0, w3)
                m.bottom[k, :, lanes] = run(h3 - 2 + k, 0, w3)
                m.el[k, :, lanes] = column(k)
                m.er[k, :, lanes] = column(w3 - 2 + k)
                for corner, (r, c) in enumerate(((0, 0), (0, w3 - 2), (h3 - 2, 0), (h3 - 2, w3 - 2))):
                    m.cs[corner, 2 * k:2 * k + 2, lanes] = run(r + k, c, 2)
        send(m)

    def assemble_small(m):
        receive(m, range(8))
        for t, lo, n in lane_tiles(m.channels):
            tile = f3.at[t]
            lanes = slice(lo, lo + n)
            for k in range(2):
                def put_run(r, c, value):
                    tile[at_pixel(r, c):at_pixel(r, c) + value.shape[0], :] = value.astype(F32)

                put_run(k - 2, 0, m.above[k, :, lanes])
                put_run(h3 + k, 0, m.below[k, :, lanes])
                tile[pl.ds(at_pixel(0, k - 2), h3, stride=stride), :] = m.hl[k, :, lanes].astype(F32)
                tile[pl.ds(at_pixel(0, w3 + k), h3, stride=stride), :] = m.hr[k, :, lanes].astype(F32)
                for corner, (r, c) in enumerate(((-2, -2), (-2, w3), (h3, -2), (h3, w3))):
                    put_run(r + k, c, m.cr[corner, :, lanes].astype(F32)[2 * k:2 * k + 2])
            x3[:, lanes] = tile[...].astype(BF16)

    def conv_small(src, count, cin, taps, bias, which, store):
        main, rest = split(half)

        def lhs():
            return packed_lhs([src[dy * stride:dy * stride + count, :] for dy in range(3)], cin)

        def step(dx, carry):
            bscr[dx, :count, :main] = dots(lhs(), taps.columns(dx), False)
            return carry

        for dx in range(3):
            step(dx, 0)
        bscr[3, :count, :3 * rest] = dots(lhs(), taps.last_columns(), False)
        for t, lo, n in lane_tiles(half):
            if lo < main:
                parts = [bscr[dx, :count, lo:lo + n] for dx in range(3)]
            else:
                parts = [bscr[3, :count, dx * rest:(dx + 1) * rest] for dx in range(3)]
            value = parts[0] + pltpu.roll(parts[1], count - 1, 0) + pltpu.roll(parts[2], count - 2, 0)
            at = which * half + lo
            store(at, jnp.maximum(value + bias[at:at + n][None, :], 0.0))

    for t, lo, n in lane_tiles(c2):
        value = pooled(acc2, t, h2, w2)
        for r in range(h3):
            f3[t, at_pixel(r, 0):at_pixel(r, 0) + w3, :] = value[r * w3:(r + 1) * w3]
    send_small(mp2)
    put_edges(ms2, acc2)
    send(ms2)

    def skip_sum(t):
        return acc_skip.at[t], 0

    load("d2s").wait()
    skip_taps = Taps(buf_f, c2, c2)
    conv_sum(ms2, skip_taps, c2, skip_sum, dys=(1,), halo=False)
    load("ma0").wait()
    load("ma1").wait()
    assemble_small(mp2)

    place = lax.broadcasted_iota(jnp.int32, (wide, 1), 0)
    line, spot = place // stride, place % stride
    inside = ((line >= 1 - has(-1, 0).astype(jnp.int32)) & (line <= h3 + has(1, 0).astype(jnp.int32))
              & (spot >= 1 - has(0, -1).astype(jnp.int32)) & (spot <= w3 + has(0, 1).astype(jnp.int32)))

    def keep_padded(lo, value):
        x3b[:, lo:lo + LANE] = jnp.where(inside, value, 0.0).astype(BF16)

    def keep_flat(lo, value):
        m3[:, lo:lo + LANE] = value.astype(BF16)

    for which in range(2):
        conv_small(x3, wide, c2, Taps(buf_d, c2, half, first=9 * which), bma, which, keep_padded)
        load(("mb1", "mb2")[which]).start()
    load("mb0").wait()
    conv_small(x3b, own, c3, Taps(buf_e, c3, half, fold=2), bmb, 0, keep_flat)
    load("d2u").start()
    load("mb1").wait()
    load("mb2").wait()
    conv_small(x3b, own, c3, Taps(buf_d, c3, half, fold=2), bmb, 1, keep_flat)
    load("d2b").start()
    load("u1").start()

    load("u2").wait()
    for p in range(2):
        for q in range(2):
            at = 2 * (2 * p + q)
            value = mm(m3[...], buf_c[at:at + 2].reshape(c3, c2), False)
            for t, lo, n in lane_tiles(c2):
                bscr[0, :own, :LANE] = value[:, lo:lo + n]
                tile = acc2.at[t]
                for r in range(h3):
                    tile[pl.ds((2 * r + p) * w2 + q, w3, stride=2), :] = bscr[0, r * stride:r * stride + w3, :LANE]
    for t, lo, n in lane_tiles(c2):
        mu2.x[1:h2 + 1, :, lo:lo + n] = acc2[t].astype(BF16).reshape(h2, w2, n)
    put_edges(mu2, acc2)
    send(mu2)
    conv_sum(ms2, skip_taps, c2, skip_sum, dys=(0, 2), add=True)
    load("d2u").wait()
    conv_mid(mu2, Taps(buf_e, c2, c2), c2, bd2a, keep_in(md2), partial=skip_sum)
    put_edges(md2, acc2)
    send(md2)
    load("d1b").wait()
    taps.pack()
    load("d2b").wait()

    def keep_d2(begin, count, t, value):
        d2buf[:, t * LANE:(t + 1) * LANE] = value.astype(BF16)

    conv_mid(md2, Taps(buf_d, c2, c2), c2, bd2b, keep_d2)

    load("u1").wait()
    for at in range(4):
        bscr[at, :h2 * w2, :c1] = mm(d2buf[...], buf_d[9 + at // 2, (at % 2) * c1:(at % 2 + 1) * c1, :], True)
    quarter = h1 // 4
    for t, lo, n in lane_tiles(c1):
        for r in range(h2):
            tile = acc2.at[2 * r // quarter]
            for at in range(4):
                begin = (2 * r % quarter + at // 2) * w1 + at % 2
                tile[pl.ds(begin, w2, stride=2), :] = bscr[at, r * w2:(r + 1) * w2, lo:lo + LANE]
        ends = []
        for k in range(4):
            tile = acc2.at[k]
            mu1.x[1 + k * quarter:1 + (k + 1) * quarter, :, lo:lo + n] = tile[:, :n].astype(BF16).reshape(quarter, w1, n)
            left = tile[pl.ds(0, quarter, stride=w1), :]
            right = tile[pl.ds(w1 - 1, quarter, stride=w1), :]
            put_columns(mu1, slice(k * quarter, (k + 1) * quarter), left, right, in_order(t, lo, n))
            ends.append((left, right))
        (first_left, first_right), (last_left, last_right) = ends[0], ends[-1]
        put_corners(mu1, (first_left[:1], first_right[:1], last_left[quarter - 1:], last_right[quarter - 1:]),
                    in_order(t, lo, n))
    send(mu1)
    load("d1a").wait()
    conv_large(mu1, TapsT(buf_b, c1, c1, (0, split(c1)[0])), c1, acc1, bd1a, keep_in(md1), add=True)
    put_edges(md1, acc1)
    send(md1)

    def keep_last(begin, count, t, value):
        lo = t * LANE
        ma1.x[pl.ds(1 + begin, count), :, lo:lo + value.shape[1]] = value.astype(BF16).reshape(count, w1, value.shape[1])

    for d in range(8):
        @pl.when(has(*DIRS[d]))
        def _(d=d):
            remote(ma1, d).wait_send()
    conv_large(md1, taps, c1, acc1, bd1b, keep_last)

    for b in range(4):
        count = h1 // 4
        last = ma1.x[1 + b * count:1 + (b + 1) * count].reshape(count * w1, c1)
        y = mm(wh[...], last, True)
        for r in range(count):
            for o in range(wh.shape[0]):
                out[b * count + r, o:o + 1] = y[o:o + 1, r * w1:(r + 1) * w1] + bh[o]

    for m in maps:
        if m is ma1:
            continue
        for d in range(8):
            @pl.when(has(*DIRS[d]))
            def _(m=m, d=d):
                remote(m, d).wait_send()


def solution(mesh):
    rows, cols = mesh.shape["row"], mesh.shape["col"]
    tile_spec = P(("data", "row"), "col", None)

    def device_body(image, w1a, b1a, w1b, b1b, w2a, b2a, w2b, b2b, wma, bma, wmb, bmb, wu2, wd2a, bd2a, wd2b, bd2b,
                    wu1, wd1a, bd1a, wd1b, bd1b, wh, bh):
        h1, w1, cin = image.shape
        c1, c2, c3 = w1b.shape[3], w2b.shape[3], wmb.shape[3]
        couts = wh.shape[1]
        h2, w2, h3, w3 = h1 // 2, w1 // 2, h1 // 4, w1 // 4

        def stack(w):
            return w.reshape(-1, min(w.shape[2], c2), w.shape[3])

        def stack_t(w):
            return jnp.swapaxes(w, 2, 3).reshape(-1, w.shape[3], w.shape[2])

        operands = [image, w1a.reshape(9, cin, c1), b1a, stack(w1b), b1b, stack(w2a), b2a, stack(w2b), b2b,
                    stack(wma), bma, stack(wmb), bmb, stack(wu2), wd2a.reshape(9, 2 * c2, c2), bd2a, stack(wd2b), bd2b,
                    stack_t(wu1).reshape(2, 2 * c1, c2), stack_t(wd1a), bd1a, stack(wd1b), bd1b, wh.T, bh]
        in_vmem = {0, 23, 24}
        vmem = pl.BlockSpec(memory_space=pltpu.VMEM)
        hbm = pl.BlockSpec(memory_space=pl.ANY)
        nt1, nt2 = -(-c1 // LANE), c2 // LANE
        small = 2 * w3
        specs = map_specs(h1, w1, cin, c1, c2)
        scratch = (
            [shape for spec in specs for shape in map_scratch(*spec)]
            + [
                pltpu.VMEM((nt1, h1 * w1, LANE), F32), *[pltpu.VMEM((nt2, h2 * w2, LANE), F32)] * 2,
                pltpu.VMEM((4, h2 * w2 + 2 * h2, split(c2)[0]), F32), pltpu.VMEM((h1 + 16, c2), F32),
                pltpu.VMEM((3, 2 * h2, c2), BF16),
                pltpu.VMEM((nt2, (h3 + 4) * small, LANE), F32), pltpu.VMEM(((h3 + 4) * small, c2), BF16),
                pltpu.VMEM(((h3 + 2) * small, c3), BF16),
                pltpu.VMEM((h3 * small, c3), BF16), pltpu.VMEM((h2 * w2, c2), BF16),
                pltpu.VMEM((9, c1, c1), BF16), pltpu.VMEM((9, c1, c2), BF16), pltpu.VMEM((9, c2, c2), BF16),
                pltpu.VMEM((18, c2, c2), BF16), pltpu.VMEM((18, c2, c2), BF16), pltpu.VMEM((9, c2, c2), BF16),
                pltpu.VMEM((3, c1, 3 * split(c1)[1]), BF16),
                pltpu.VMEM((3, 16, c1), BF16), pltpu.VMEM((16, 3 * split(c1)[1]), BF16),
                pltpu.VMEM((9, cin, c1), BF16),
                *[pltpu.VMEM((c,), F32) for c in (c1, c1, c2, c2, c3, c3, c2, c2, c1, c1)],
                *[pltpu.SemaphoreType.DMA((len(specs), len(DIRS)))] * 2, pltpu.SemaphoreType.DMA((27,)),
            ]
        )
        y = pl.pallas_call(
            functools.partial(unet_kernel, (h1, w1, cin, c1, c2, c3, rows, cols)),
            out_shape=jax.ShapeDtypeStruct((h1, couts, w1), F32),
            in_specs=[vmem if i in in_vmem else hbm for i in range(24)] + [pl.BlockSpec(memory_space=pltpu.SMEM)],
            out_specs=vmem,
            scratch_shapes=scratch,
            compiler_params=pltpu.CompilerParams(collective_id=0, has_side_effects=True, vmem_limit_bytes=67043328),
            name="unet",
        )(*operands)
        return y.transpose(0, 2, 1)

    def program(image, *params):
        mapped = jax.shard_map(device_body, mesh=mesh, in_specs=(tile_spec,) + tuple([P()] * len(params)),
                               out_specs=tile_spec, check_vma=False)
        return mapped(image, *params)

    return program
```
